32 devices in a mesh: rep: 8 (over z, x), tp: 4 (over y, core).
Axes of the slice: x: 2, y: 2, z: 4, core: 2. Of those that a mesh axis runs over, the one named last changes fastest.
Arguments:
- tokens: bfloat16 [64, 4096], P(('rep', 'tp')), may hold values from -6 to 6
- conv_state: bfloat16 [3, 64, 8192], P(None, 'rep', 'tp'), may hold values from -6 to 6
- ssm_state: float32 [64, 16, 8192], P('rep', None, 'tp'), may hold values from -6 to 6
- norm_gains: bfloat16 [2, 4096], P(None, ('rep', 'tp')), may hold values from 0.5 to 1.5
- conv_weight: bfloat16 [4, 8192], P(None, ('rep', 'tp')), may hold values from -3 to 3
- conv_skip: bfloat16 [2, 8192], P(None, ('rep', 'tp')), may hold values from -3 to 3
- step_bias: bfloat16 [8192], P(('rep', 'tp')), may hold values from -5 to -1
- decay_log: bfloat16 [16, 8192], P(None, ('rep', 'tp')), may hold values from 0 to 2.796875
- input_proj: bfloat16 [4096, 2, 8192], P(('rep', 'tp')), may hold values from -0.09375 to 0.09375
- select_proj: bfloat16 [8192, 288], P('tp', 'rep'), may hold values from -0.0625 to 0.0625
- step_proj: bfloat16 [256, 8192], P(('rep', 'tp')), may hold values from -0.375 to 0.375
- output_proj: bfloat16 [8192, 4096], P(None, ('rep', 'tp')), may hold values from -0.0625 to 0.0625
- router: bfloat16 [4096, 16], P(('rep', 'tp')), may hold values from -0.09375 to 0.09375
- expert_proj: bfloat16 [4096, 2, 2, 12288], P(('rep', 'tp')), may hold values from -0.09375 to 0.09375
- expert_ids: int32 [64, 2], P(('rep', 'tp')), may hold values from 0 to 15, as said below
Outputs:
- mamba_out: bfloat16 [64, 4096], P(('rep', 'tp'))
- conv_next: bfloat16 [3, 64, 8192], P(None, 'rep', 'tp')
- ssm_next: float32 [64, 16, 8192], P('rep', None, 'tp')
- expert_hidden: bfloat16 [128, 12288], P('rep', 'tp')
The draws below stay inside these ranges and needn't reach their ends.
Inputs may be any that keep to these rules, and one draw needn't show every extreme that they name: `expert_ids`: each row names two different experts. Within each aligned block of 2 rows (the rows of one device) each expert e < 2 is named by at most 2 rows.
All inputs are finite; a program needn't handle non-finite values.
Results may differ from the reference program's by a relative error of at most 0.04.
Values may be sent and summed in bfloat16 or wider, within the bound.
A program may use at most 192 MiB of HBM per device.

```python
import jax
import jax.numpy as jnp
from jax import lax

D = 4096
INNER = 8192
STEP_RANK = 256
STATE = 16
TAPS = 4
FF = 12288
EXPERTS = 16
EXP_WIN = 2
CAPACITY = 2
TOK_DEV = 2
REQ = 8
TOKENS = 64
SLOTS = 128
N_REP = 8
N_TP = 4


def draw_expert_ids(key, part):
    blocks = TOKENS // TOK_DEV
    per_replica = REQ // TOK_DEV
    subkeys = jax.random.split(jax.random.fold_in(key, 17), 6)
    counts = jax.random.randint(subkeys[0], (blocks, EXP_WIN), 1, CAPACITY + 1)
    full_replica = jax.random.randint(subkeys[1], (), 0, blocks // per_replica)
    replica_of = jnp.arange(blocks, dtype=jnp.int32) // per_replica
    counts = jnp.where((replica_of == full_replica)[:, None], CAPACITY, counts)
    scores = jax.random.randint(subkeys[2], (blocks, TOK_DEV, EXP_WIN), 0, 1 << 20) * TOK_DEV + jnp.arange(TOK_DEV, dtype=jnp.int32)[None, :, None]
    ordering = jnp.argsort(scores, axis=1)
    order_rank = jnp.argsort(ordering, axis=1)
    member = order_rank < counts[:, None, :]
    in_first = member[:, :, 0]
    in_second = member[:, :, 1]
    spare = EXPERTS - EXP_WIN
    spare_one = EXP_WIN + jax.random.randint(subkeys[3], (blocks, TOK_DEV), 0, spare)
    spare_two = EXP_WIN + (spare_one - EXP_WIN + jax.random.randint(subkeys[4], (blocks, TOK_DEV), 1, spare)) % spare
    first_pick = jnp.where(in_first, 0, jnp.where(in_second, 1, spare_one))
    second_pick = jnp.where(in_first & in_second, 1, jnp.where(in_first | in_second, spare_one, spare_two))
    swapped = jax.random.randint(subkeys[5], (blocks, TOK_DEV), 0, 2) == 1
    column_one = jnp.where(swapped, second_pick, first_pick)
    column_two = jnp.where(swapped, first_pick, second_pick)
    return jnp.stack([column_one, column_two], axis=-1).reshape(TOKENS, 2).astype(jnp.int32)


def shard_levels(key, extent, cuts, least, top_value):
    def one(axis_at, blocks):
        draws = jax.random.uniform(jax.random.fold_in(jax.random.fold_in(key, 6), axis_at), (blocks,), jnp.float32, least / len(cuts), top_value / len(cuts))
        return jnp.repeat(jnp.exp(draws), extent[axis_at] // blocks).reshape((-1,) + (1,) * (len(extent) - axis_at - 1))

    level = one(*cuts[0])
    for cut in cuts[1:]:
        level = level * one(*cut)
    return level


def normal_values(own_key, dims, scale, bound, cuts=(), held_as=jnp.bfloat16):
    level = shard_levels(own_key, dims, cuts, -0.22, 0.18) if cuts else 1.0
    array = jax.random.normal(own_key, dims, jnp.float32) * scale * level
    return jnp.minimum(jnp.maximum(array, -bound), bound).astype(held_as)


def setup_inputs(seed: int = 0) -> dict:
    splits = jax.random.split(jax.random.key(seed), 16)
    return {
        "tokens": normal_values(splits[0], (TOKENS, D), 1.0, 6.0, ((0, 32),)),
        "conv_state": normal_values(splits[1], (TAPS - 1, TOKENS, INNER), 1.0, 6.0, ((1, 8), (2, 4))),
        "ssm_state": normal_values(splits[2], (TOKENS, STATE, INNER), 1.0, 6.0, ((0, 8), (2, 4)), jnp.float32),
        "norm_gains": jnp.clip(1.0 + 0.1 * jax.random.normal(splits[3], (2, D), jnp.float32), 0.5, 1.5).astype(jnp.bfloat16),
        "conv_weight": normal_values(splits[4], (TAPS, INNER), 0.5, 3.0, ((1, 32),)),
        "conv_skip": normal_values(splits[5], (2, INNER), 0.5, 3.0, ((1, 32),)),
        "step_bias": jnp.clip(-5.0 + 4.0 * jax.random.uniform(splits[6], (INNER,), jnp.float32) ** shard_levels(splits[6], (INNER,), ((0, 32),), -0.2, 0.2), -5.0, -1.0).astype(jnp.bfloat16),
        "decay_log": jnp.clip(2.796875 * jax.random.uniform(splits[7], (STATE, INNER), jnp.float32) ** shard_levels(splits[7], (STATE, INNER), ((1, 32),), -0.2, 0.2), 0.0, 2.796875).astype(jnp.bfloat16),
        "input_proj": normal_values(splits[8], (D, 2, INNER), D ** -0.5, 0.09375, ((0, 32),)),
        "select_proj": normal_values(splits[9], (INNER, STEP_RANK + 2 * STATE), INNER ** -0.5, 0.0625, ((0, 4), (1, 8))),
        "step_proj": normal_values(splits[10], (STEP_RANK, INNER), STEP_RANK ** -0.5, 0.375, ((0, 32),)),
        "output_proj": normal_values(splits[11], (INNER, D), INNER ** -0.5, 0.0625, ((1, 32),)),
        "router": normal_values(splits[12], (D, EXPERTS), D ** -0.5, 0.09375, ((0, 32),)),
        "expert_proj": normal_values(splits[13], (D, EXP_WIN, 2, FF), D ** -0.5, 0.09375, ((0, 32),)),
        "expert_ids": draw_expert_ids(jax.random.fold_in(splits[15], 71), 0),
    }


epsilon = 1e-05

def norm_scale(values, gain):
    mean_square = lax.optimization_barrier(jnp.mean(values * values, axis=-1, keepdims=True))
    return values * lax.rsqrt(mean_square + epsilon) * gain.astype(jnp.float32)

def ssm_block(block_args):
    state, step_size, activated, input_map, output_map, decay_rate = block_args
    factor = jnp.exp(step_size[:, None, :] * decay_rate[None])
    state_next = factor * state + (step_size * activated)[:, None, :] * input_map[:, :, None]
    readout = lax.optimization_barrier(jnp.sum(state_next * output_map[:, :, None], axis=1))
    return (state_next, readout)

def reference(tokens, conv_state, ssm_state, norm_gains, conv_weight, conv_skip, step_bias, decay_log, input_proj, select_proj, step_proj, output_proj, router, expert_proj, expert_ids):
    residual_in = tokens.astype(jnp.float32)
    normed = norm_scale(residual_in, norm_gains[0]).astype(jnp.bfloat16)
    projected = jnp.dot(normed, input_proj.reshape(D, 2 * INNER), preferred_element_type=jnp.float32)
    conv_input = projected[:, :INNER]
    gate_z = projected[:, INNER:]
    conv_taps = conv_weight.astype(jnp.float32)
    history = conv_state.astype(jnp.float32)
    conv_mix = lax.optimization_barrier(jnp.sum(conv_taps[:-1, None, :] * history, axis=0)) + conv_taps[-1] * conv_input + conv_skip[0].astype(jnp.float32)
    conv_next = jnp.concatenate([conv_state[1:], conv_input.astype(jnp.bfloat16)[None]], axis=0)
    activated = jax.nn.silu(conv_mix)
    selected = jnp.dot(activated.astype(jnp.bfloat16), select_proj, preferred_element_type=jnp.float32)
    step_low = selected[:, :STEP_RANK].astype(jnp.bfloat16)
    input_map = selected[:, STEP_RANK:STEP_RANK + STATE]
    output_map = selected[:, STEP_RANK + STATE:]
    step_size = jax.nn.softplus(jnp.dot(step_low, step_proj, preferred_element_type=jnp.float32) + step_bias.astype(jnp.float32))
    decay_rate = -jnp.exp(decay_log.astype(jnp.float32))
    replicas = TOKENS // REQ
    state_next, readout = lax.map(lambda block_args: ssm_block(block_args + (decay_rate,)), (ssm_state.reshape(replicas, REQ, STATE, INNER), step_size.reshape(replicas, REQ, INNER), activated.reshape(replicas, REQ, INNER), input_map.reshape(replicas, REQ, STATE), output_map.reshape(replicas, REQ, STATE)))
    ssm_next = state_next.reshape(TOKENS, STATE, INNER)
    readout = readout.reshape(TOKENS, INNER) + conv_skip[1].astype(jnp.float32) * activated
    gated_out = (readout * jax.nn.silu(gate_z)).astype(jnp.bfloat16)
    inner_block = INNER // N_TP
    mixer_out = jnp.zeros((TOKENS, D), jnp.float32)
    for block_index in range(N_TP):
        lower = block_index * inner_block
        partial_out = jnp.dot(gated_out[:, lower:lower + inner_block], output_proj[lower:lower + inner_block], preferred_element_type=jnp.float32)
        mixer_out = mixer_out + lax.optimization_barrier(partial_out.astype(jnp.bfloat16)).astype(jnp.float32)
    residual = residual_in + mixer_out
    mamba_out = residual.astype(jnp.bfloat16)
    moe_in = norm_scale(residual, norm_gains[1]).astype(jnp.bfloat16)
    logits = jnp.dot(moe_in, router, preferred_element_type=jnp.float32)
    choose = (expert_ids[:, :, None] == jnp.arange(EXPERTS, dtype=jnp.int32)[None, None, :]).astype(jnp.float32)
    picked = lax.optimization_barrier(jnp.sum(choose * logits[:, None, :], axis=2))
    first_gate = jax.nn.sigmoid(picked[:, 0] - picked[:, 1])
    second_gate = jax.nn.sigmoid(picked[:, 1] - picked[:, 0])
    window = jnp.arange(EXP_WIN, dtype=jnp.int32)
    names_first = expert_ids[:, 0:1] == window[None, :]
    names_second = expert_ids[:, 1:2] == window[None, :]
    zero = jnp.zeros((), jnp.float32)
    gate_w = jnp.where(names_first, first_gate[:, None], zero) + jnp.where(names_second, second_gate[:, None], zero)
    routed = (names_first | names_second).astype(jnp.int32)
    blocks = TOKENS // TOK_DEV
    routed_blocks = routed.reshape(blocks, TOK_DEV, EXP_WIN)
    position = jnp.cumsum(routed_blocks, axis=1) - routed_blocks
    slot_of = ((position[..., None] == jnp.arange(CAPACITY, dtype=jnp.int32)) & (routed_blocks[..., None] > 0)).astype(jnp.float32)
    slot_x = jnp.einsum('btec,btd->becd', slot_of, moe_in.reshape(blocks, TOK_DEV, D).astype(jnp.float32)).astype(jnp.bfloat16)
    slot_gate = jnp.einsum('btec,bte->bec', slot_of, gate_w.reshape(blocks, TOK_DEV, EXP_WIN)).astype(jnp.bfloat16)
    feature_block = D // N_REP
    hidden_list = []
    for expert in range(EXP_WIN):
        slot_rows = slot_x[:, expert].reshape(blocks * CAPACITY, D)
        gate_up = jnp.zeros((blocks * CAPACITY, 2 * FF), jnp.float32)
        for block_index in range(N_REP):
            lower = block_index * feature_block
            partial_up = jnp.dot(slot_rows[:, lower:lower + feature_block], expert_proj[lower:lower + feature_block, expert].reshape(feature_block, 2 * FF), preferred_element_type=jnp.float32)
            gate_up = gate_up + lax.optimization_barrier(partial_up.astype(jnp.bfloat16)).astype(jnp.float32)
        slot_scale = slot_gate[:, expert].reshape(blocks * CAPACITY).astype(jnp.float32)
        hidden = slot_scale[:, None] * jax.nn.silu(gate_up[:, :FF]) * gate_up[:, FF:]
        hidden_list.append(hidden.reshape(blocks, CAPACITY, FF))
    expert_hidden = jnp.stack(hidden_list, axis=1).reshape(SLOTS, FF).astype(jnp.bfloat16)
    return (mamba_out, conv_next, ssm_next, expert_hidden)
```

```python
import jax
import jax.numpy as jnp
from jax import lax
from jax.sharding import PartitionSpec as P

CAPACITY = 2
LANES = 128


epsilon = 1e-05


def shards(
    tokens,
    conv_state,
    ssm_state,
    norm_gains,
    conv_weight,
    conv_skip,
    step_bias,
    decay_log,
    input_proj,
    select_proj,
    step_proj,
    output_proj,
    router,
    expert_proj,
    expert_ids,
):
    f32, bf16 = jnp.float32, jnp.bfloat16
    both = ("rep", "tp")
    tp_count = lax.axis_size("tp")
    rep_count = lax.axis_size("rep")
    count = tp_count * rep_count
    tp_index = lax.axis_index("tp")
    rep_index = lax.axis_index("rep")
    tok_dev, width = tokens.shape
    slice_dev = width // count
    token_count = tok_dev * count
    req = tok_dev * tp_count
    inner_all = input_proj.shape[2]
    inner_dev = ssm_state.shape[2]
    state_count = ssm_state.shape[1]
    step_rank = step_proj.shape[0] * count
    expert_total = router.shape[1]
    window_count = expert_proj.shape[1]

    tok = tokens.astype(f32)
    scale = lax.rsqrt(jnp.mean(tok * tok, axis=-1, keepdims=True) + epsilon)
    extra = jnp.concatenate([scale, expert_ids.astype(f32)], axis=1)
    extra = jnp.pad(extra, ((0, 0), (0, LANES - 3)))
    sent = jnp.concatenate(
        [
            tok.reshape(tok_dev, count, slice_dev),
            jnp.broadcast_to(extra[:, None, :], (tok_dev, count, LANES)),
        ],
        axis=2,
    ).transpose(1, 0, 2)
    got = lax.all_to_all(sent, both, split_axis=0, concat_axis=0, tiled=True)
    got = got.reshape(token_count, slice_dev + LANES)
    tok_slice = got[:, :slice_dev]
    scale_all = got[:, slice_dev : slice_dev + 1]
    ids_all = got[:, slice_dev + 1 : slice_dev + 3].astype(jnp.int32)

    gains = norm_gains.astype(f32)
    normed = (tok_slice * scale_all * gains[0]).astype(bf16)
    partial_in = jnp.dot(
        normed, input_proj.reshape(slice_dev, 2 * inner_all), preferred_element_type=f32
    ).astype(bf16)
    partial_in = partial_in.reshape(token_count, 2, inner_all)
    partial_in = lax.psum_scatter(partial_in, "rep", scatter_dimension=0, tiled=True)
    partial_in = lax.psum_scatter(partial_in, "tp", scatter_dimension=2, tiled=True)
    conv_input = partial_in[:, 0].astype(f32)
    gate_z = partial_in[:, 1].astype(f32)

    packed = jnp.concatenate([conv_weight, conv_skip, step_bias[None], decay_log], axis=0)
    packed = lax.all_gather(packed, both, axis=1, tiled=True)
    packed = lax.dynamic_slice_in_dim(packed, tp_index * inner_dev, inner_dev, 1).astype(f32)
    taps = conv_weight.shape[0]
    conv_taps = packed[:taps]
    skip_rows = packed[taps : taps + 2]
    shift_dev = packed[taps + 2]
    decay_dev = packed[taps + 3 :]
    step_rows = lax.all_to_all(
        step_proj.reshape(step_proj.shape[0], tp_count, inner_dev),
        "tp",
        split_axis=1,
        concat_axis=0,
        tiled=True,
    )
    step_rows = lax.all_gather(
        step_rows.reshape(tp_count * step_proj.shape[0], inner_dev), "rep", axis=0, tiled=True
    )
    select_rows = lax.all_gather(select_proj, "rep", axis=1, tiled=True)

    history = conv_state.astype(f32)
    conv_mix = (
        jnp.sum(conv_taps[:-1, None, :] * history, axis=0)
        + conv_taps[-1] * conv_input
        + skip_rows[0]
    )
    conv_next = jnp.concatenate([conv_state[1:], partial_in[:, 0][None]], axis=0)
    activated = jax.nn.silu(conv_mix)
    select_part = jnp.dot(activated.astype(bf16), select_rows, preferred_element_type=f32)
    selected = lax.psum(select_part.astype(bf16), "tp").astype(f32)
    step_low = selected[:, :step_rank].astype(bf16)
    input_map = selected[:, step_rank : step_rank + state_count]
    output_map = selected[:, step_rank + state_count :]
    step_size = jax.nn.softplus(
        jnp.dot(step_low, step_rows, preferred_element_type=f32) + shift_dev
    )
    decay_rate = -jnp.exp(decay_dev)
    factor = jnp.exp(step_size[:, None, :] * decay_rate[None])
    ssm_next = factor * ssm_state + (step_size * activated)[:, None, :] * input_map[:, :, None]
    readout = jnp.sum(ssm_next * output_map[:, :, None], axis=1) + skip_rows[1] * activated
    gated_out = (readout * jax.nn.silu(gate_z)).astype(bf16)

    gated_all = lax.all_gather(gated_out, both, axis=0, tiled=False)
    gated_all = gated_all.reshape(rep_count, tp_count, req, inner_dev)
    gated_all = gated_all.transpose(0, 2, 1, 3).reshape(token_count, inner_all)
    mixer_out = jnp.dot(gated_all, output_proj, preferred_element_type=f32)
    residual = tok_slice + mixer_out
    home = residual.astype(bf16).reshape(count, tok_dev, slice_dev)
    home = lax.all_to_all(home, both, split_axis=0, concat_axis=0, tiled=True)
    mamba_out = home.transpose(1, 0, 2).reshape(tok_dev, width)

    gained = residual * gains[1]
    logit_part = jnp.dot(
        gained, router.astype(f32), preferred_element_type=f32, precision=lax.Precision.HIGHEST
    )
    square_part = jnp.sum(residual * residual, axis=1, keepdims=True)
    summed = lax.psum(jnp.concatenate([logit_part, square_part], axis=1), both)
    scale_two = lax.rsqrt(summed[:, expert_total:] / width + epsilon)
    logits = summed[:, :expert_total] * scale_two
    moe_in = (gained * scale_two).astype(bf16)

    choose = (
        ids_all[:, :, None] == jnp.arange(expert_total, dtype=jnp.int32)[None, None, :]
    ).astype(f32)
    picked = jnp.sum(choose * logits[:, None, :], axis=2)
    first_gate = jax.nn.sigmoid(picked[:, 0] - picked[:, 1])
    second_gate = jax.nn.sigmoid(picked[:, 1] - picked[:, 0])
    window = jnp.arange(window_count, dtype=jnp.int32)
    names_first = ids_all[:, 0:1] == window[None, :]
    names_second = ids_all[:, 1:2] == window[None, :]
    zero = jnp.zeros((), f32)
    gate_w = jnp.where(names_first, first_gate[:, None], zero) + jnp.where(
        names_second, second_gate[:, None], zero
    )
    routed = (names_first | names_second).astype(jnp.int32)
    routed = routed.reshape(count, tok_dev, window_count)
    position = jnp.cumsum(routed, axis=1) - routed
    slot_of = (position[..., None] == jnp.arange(CAPACITY, dtype=jnp.int32)) & (
        routed[..., None] > 0
    )
    slot_of = slot_of.astype(f32)
    blocks_x = moe_in.reshape(count, tok_dev, slice_dev).astype(f32)
    slot_x = jnp.sum(slot_of[..., None] * blocks_x[:, :, None, None, :], axis=1).astype(bf16)
    slot_gate = jnp.sum(slot_of * gate_w.reshape(count, tok_dev, window_count)[..., None], axis=1)
    slot_gate = slot_gate.astype(bf16)

    expert_blocks = lax.all_to_all(expert_proj, "tp", split_axis=3, concat_axis=0, tiled=True)
    hidden_dev = expert_blocks.shape[3]
    slot_rows = lax.all_gather(slot_x, "tp", axis=3, tiled=True)
    product = jnp.einsum(
        "gecd,dexf->gecxf", slot_rows, expert_blocks, preferred_element_type=f32
    ).astype(bf16)
    slot_count = count * window_count * CAPACITY
    summed = lax.psum_scatter(
        product.reshape(slot_count, 2 * hidden_dev), "rep", scatter_dimension=0, tiled=True
    ).astype(f32)
    own = slot_count // rep_count
    gate_own = lax.dynamic_slice_in_dim(slot_gate.reshape(slot_count), rep_index * own, own, 0)
    hidden = (
        gate_own.astype(f32)[:, None]
        * jax.nn.silu(summed[:, :hidden_dev])
        * summed[:, hidden_dev:]
    )
    expert_hidden = hidden.astype(bf16)
    return (mamba_out, conv_next, ssm_next, expert_hidden)


def solution(mesh):
    in_specs = (
        P(("rep", "tp"), None),
        P(None, "rep", "tp"),
        P("rep", None, "tp"),
        P(None, ("rep", "tp")),
        P(None, ("rep", "tp")),
        P(None, ("rep", "tp")),
        P(("rep", "tp")),
        P(None, ("rep", "tp")),
        P(("rep", "tp"), None, None),
        P("tp", "rep"),
        P(("rep", "tp"), None),
        P(None, ("rep", "tp")),
        P(("rep", "tp"), None),
        P(("rep", "tp"), None, None, None),
        P(("rep", "tp"), None),
    )
    out_specs = (P(("rep", "tp"), None), P(None, "rep", "tp"), P("rep", None, "tp"), P("rep", "tp"))
    return jax.shard_map(shards, mesh=mesh, in_specs=in_specs, out_specs=out_specs, check_vma=False)
```

```python
import functools

import jax
import jax.numpy as jnp
from jax import lax
from jax.experimental import pallas as pl
from jax.experimental.pallas import tpu as pltpu
from jax.sharding import PartitionSpec as P

CAPACITY = 2
LANES = 128


epsilon = 1e-05
MESH = pl.DeviceIdType.MESH


def send_kernel(plan, *refs):
    arrays = len(plan)
    sources, targets, sems = refs[:arrays], refs[arrays : 2 * arrays], refs[2 * arrays :]
    barrier = pltpu.get_barrier_semaphore()
    greeted = 0
    for axis, count in dict((axis, count) for axis, count, _ in plan).items():
        me = lax.axis_index(axis)
        for step in range(1, count):
            pl.semaphore_signal(
                barrier, inc=1, device_id={axis: lax.rem(me + step, count)}, device_id_type=MESH
            )
        greeted += count - 1
    pl.semaphore_wait(barrier, greeted)
    copies = []
    for which, (axis, count, mode) in enumerate(plan):
        me = lax.axis_index(axis)
        for step in range(1, count):
            peer = lax.rem(me + step, count)
            source = sources[which]
            if mode == "lanes":
                lanes = source.shape[-1] // count
                source = source.at[:, pl.ds(pl.multiple_of(peer * lanes, lanes), lanes)]
            elif mode == "lead":
                source = source.at[peer]
            copy = pltpu.make_async_remote_copy(
                src_ref=source,
                dst_ref=targets[which].at[me],
                send_sem=sems[2 * which].at[step - 1],
                recv_sem=sems[2 * which + 1].at[step - 1],
                device_id={axis: peer},
                device_id_type=MESH,
            )
            copy.start()
            copies.append(copy)
    for copy in copies:
        copy.wait()


def send(items, collective_id):
    shapes, plan, scratch = [], [], []
    for x, axis, mode in items:
        count = lax.axis_size(axis)
        if mode == "lanes":
            piece = x.shape[:-1] + (x.shape[-1] // count,)
        elif mode == "lead":
            piece = x.shape[1:]
        else:
            piece = x.shape
        shapes.append(jax.ShapeDtypeStruct((count,) + piece, x.dtype))
        plan.append((axis, count, mode))
        scratch += [pltpu.SemaphoreType.DMA((count - 1,))] * 2
    return pl.pallas_call(
        functools.partial(send_kernel, tuple(plan)),
        out_shape=shapes,
        in_specs=[pl.BlockSpec(memory_space=pl.ANY)] * len(items),
        out_specs=[pl.BlockSpec(memory_space=pl.ANY)] * len(items),
        scratch_shapes=scratch,
        compiler_params=pltpu.CompilerParams(collective_id=collective_id, has_side_effects=True),
    )(*[x for x, _, _ in items])


def own_piece(x, axis, mode):
    me = lax.axis_index(axis)
    if mode == "lanes":
        lanes = x.shape[-1] // lax.axis_size(axis)
        return lax.dynamic_slice_in_dim(x, me * lanes, lanes, x.ndim - 1)
    if mode == "lead":
        return lax.dynamic_index_in_dim(x, me, 0, keepdims=False)
    return x


def sum_of(item, got):
    total = own_piece(*item).astype(jnp.float32)
    me = lax.axis_index(item[1])
    for sender in range(got.shape[0]):
        total += jnp.where(me == sender, 0.0, got[sender].astype(jnp.float32))
    return total


def all_of(item, got):
    return lax.dynamic_update_index_in_dim(got, own_piece(*item), lax.axis_index(item[1]), 0)


def gather(x, axis, collective_id):
    item = (x, axis, "whole")
    return all_of(item, send([item], collective_id)[0])


def shards(
    tokens,
    conv_state,
    ssm_state,
    norm_gains,
    conv_weight,
    conv_skip,
    step_bias,
    decay_log,
    input_proj,
    select_proj,
    step_proj,
    output_proj,
    router,
    expert_proj,
    expert_ids,
):
    f32, bf16 = jnp.float32, jnp.bfloat16
    both = ("rep", "tp")
    tp_count = lax.axis_size("tp")
    rep_count = lax.axis_size("rep")
    count = tp_count * rep_count
    tp_index = lax.axis_index("tp")
    rep_index = lax.axis_index("rep")
    tok_dev, width = tokens.shape
    slice_dev = width // count
    token_count = tok_dev * count
    req = tok_dev * tp_count
    inner_all = input_proj.shape[2]
    inner_dev = ssm_state.shape[2]
    state_count = ssm_state.shape[1]
    step_rank = step_proj.shape[0] * count
    expert_total = router.shape[1]
    window_count = expert_proj.shape[1]

    tok = tokens.astype(f32)
    scale = lax.rsqrt(jnp.mean(tok * tok, axis=-1, keepdims=True) + epsilon)
    extra = jnp.concatenate([scale, expert_ids.astype(f32)], axis=1)
    extra = jnp.pad(extra, ((0, 0), (0, LANES - 3)))
    sent = jnp.concatenate(
        [
            tok.reshape(tok_dev, count, slice_dev),
            jnp.broadcast_to(extra[:, None, :], (tok_dev, count, LANES)),
        ],
        axis=2,
    ).transpose(1, 0, 2)
    got = lax.all_to_all(sent, both, split_axis=0, concat_axis=0, tiled=True)
    got = got.reshape(token_count, slice_dev + LANES)
    tok_slice = got[:, :slice_dev]
    scale_all = got[:, slice_dev : slice_dev + 1]
    ids_all = got[:, slice_dev + 1 : slice_dev + 3].astype(jnp.int32)

    gains = norm_gains.astype(f32)
    normed = (tok_slice * scale_all * gains[0]).astype(bf16)
    branches = input_proj.shape[1]
    diagonal = jnp.eye(branches, dtype=bf16)
    wide = (diagonal[:, None, None, :] * normed[None, :, :, None]).reshape(
        branches * token_count, slice_dev * branches
    )
    partial_in = jnp.dot(
        wide, input_proj.reshape(slice_dev * branches, inner_all), preferred_element_type=f32
    ).astype(bf16)
    packed = jnp.concatenate([conv_weight, conv_skip, step_bias[None], decay_log], axis=0)
    packed_rows = packed.shape[0]
    packed = jnp.pad(packed, ((0, -packed_rows % 16), (0, 0)))
    items = [
        (partial_in, "tp", "lanes"),
        (packed, "rep", "whole"),
        (step_proj, "rep", "whole"),
        (select_proj.T, "rep", "whole"),
    ]
    received = send(items, 0)
    partial_in = sum_of(items[0], received[0])
    packed, step_rows, select_rows = [
        all_of(item, got) for item, got in zip(items[1:], received[1:])
    ]
    select_rows = select_rows.reshape(-1, inner_dev)
    partial_in = partial_in.astype(bf16).reshape(branches, rep_count, req, inner_dev)
    items = [
        (partial_in[0], "rep", "lead"),
        (partial_in[1], "rep", "lead"),
        (packed, "tp", "whole"),
        (step_rows.reshape(-1, inner_all), "tp", "lanes"),
    ]
    received = send(items, 1)
    conv_input, gate_z = [sum_of(item, got) for item, got in zip(items[:2], received[:2])]
    packed = all_of(items[2], received[2])
    packed = packed.transpose(2, 1, 0, 3).reshape(-1, inner_all)[:packed_rows]
    step_rows = all_of(items[3], received[3])
    step_rows = step_rows.reshape(tp_count, rep_count, -1, inner_dev)
    step_rows = step_rows.transpose(1, 0, 2, 3).reshape(step_rank, inner_dev)
    packed = lax.dynamic_slice_in_dim(packed, tp_index * inner_dev, inner_dev, 1).astype(f32)
    taps = conv_weight.shape[0]
    conv_taps = packed[:taps]
    skip_rows = packed[taps : taps + 2]
    shift_dev = packed[taps + 2]
    decay_dev = packed[taps + 3 :]
    history = conv_state.astype(f32)
    conv_mix = (
        jnp.sum(conv_taps[:-1, None, :] * history, axis=0)
        + conv_taps[-1] * conv_input
        + skip_rows[0]
    )
    conv_next = jnp.concatenate([conv_state[1:], conv_input.astype(bf16)[None]], axis=0)
    activated = jax.nn.silu(conv_mix)
    select_part = lax.dot_general(
        activated.astype(bf16), select_rows, (((1,), (1,)), ((), ())), preferred_element_type=f32
    )
    selected = lax.psum(select_part.astype(bf16), "tp").astype(f32)
    step_low = selected[:, :step_rank].astype(bf16)
    input_map = selected[:, step_rank : step_rank + state_count]
    output_map = selected[:, step_rank + state_count :]
    step_size = jax.nn.softplus(
        jnp.dot(step_low, step_rows, preferred_element_type=f32) + shift_dev
    )
    decay_rate = -jnp.exp(decay_dev)
    factor = jnp.exp(step_size[:, None, :] * decay_rate[None])
    ssm_next = factor * ssm_state + (step_size * activated)[:, None, :] * input_map[:, :, None]
    readout = jnp.sum(ssm_next * output_map[:, :, None], axis=1) + skip_rows[1] * activated
    gated_out = (readout * jax.nn.silu(gate_z)).astype(bf16)

    gated_all = gather(gated_out, "rep", 2).reshape(token_count, inner_dev)
    gated_all = gather(gated_all, "tp", 3)
    gated_all = gated_all.transpose(1, 0, 2).reshape(token_count, inner_all)
    mixer_out = jnp.dot(gated_all, output_proj, preferred_element_type=f32)
    residual = tok_slice + mixer_out
    home = residual.astype(bf16).reshape(count, tok_dev, slice_dev)
    home = lax.all_to_all(home, both, split_axis=0, concat_axis=0, tiled=True)
    mamba_out = home.transpose(1, 0, 2).reshape(tok_dev, width)

    gained = residual * gains[1]
    logit_part = jnp.dot(
        gained, router.astype(f32), preferred_element_type=f32, precision=lax.Precision.HIGHEST
    )
    square_part = jnp.sum(residual * residual, axis=1, keepdims=True)
    summed = jnp.concatenate([logit_part, square_part], axis=1)
    summed = jnp.pad(summed, ((0, 0), (0, LANES - summed.shape[1])))
    summed = jnp.sum(gather(summed, "tp", 4), axis=0)
    summed = jnp.sum(gather(summed, "rep", 5), axis=0)
    scale_two = lax.rsqrt(summed[:, expert_total : expert_total + 1] / width + epsilon)
    logits = summed[:, :expert_total] * scale_two
    moe_in = (gained * scale_two).astype(bf16)

    choose = (
        ids_all[:, :, None] == jnp.arange(expert_total, dtype=jnp.int32)[None, None, :]
    ).astype(f32)
    picked = jnp.sum(choose * logits[:, None, :], axis=2)
    first_gate = jax.nn.sigmoid(picked[:, 0] - picked[:, 1])
    second_gate = jax.nn.sigmoid(picked[:, 1] - picked[:, 0])
    window = jnp.arange(window_count, dtype=jnp.int32)
    names_first = ids_all[:, 0:1] == window[None, :]
    names_second = ids_all[:, 1:2] == window[None, :]
    zero = jnp.zeros((), f32)
    gate_w = jnp.where(names_first, first_gate[:, None], zero) + jnp.where(
        names_second, second_gate[:, None], zero
    )
    routed = (names_first | names_second).astype(jnp.int32)
    routed = routed.reshape(count, tok_dev, window_count)
    position = jnp.cumsum(routed, axis=1) - routed
    slot_of = (position[..., None] == jnp.arange(CAPACITY, dtype=jnp.int32)) & (
        routed[..., None] > 0
    )
    slot_of = slot_of.astype(f32)
    blocks_x = moe_in.reshape(count, tok_dev, slice_dev).astype(f32)
    slot_x = jnp.sum(slot_of[..., None] * blocks_x[:, :, None, None, :], axis=1).astype(bf16)
    slot_gate = jnp.sum(slot_of * gate_w.reshape(count, tok_dev, window_count)[..., None], axis=1)
    slot_gate = slot_gate.astype(bf16)

    rows = count * CAPACITY
    pairs = window_count * 2
    diagonal = jnp.eye(pairs, dtype=bf16).reshape(window_count, 2, pairs)
    rows_of = slot_x.transpose(1, 0, 2, 3).reshape(window_count, rows, slice_dev)
    wide = diagonal[:, :, None, None, :] * rows_of[:, None, :, :, None]
    partial_up = jnp.dot(
        wide.reshape(pairs * rows, slice_dev * pairs),
        expert_proj.reshape(slice_dev * pairs, expert_proj.shape[3]),
        preferred_element_type=f32,
    ).astype(bf16)
    hidden_dev = expert_proj.shape[3] // tp_count
    own = rows // rep_count
    gate_up, waiting = [], []
    for expert in range(window_count + 1):
        items = list(waiting)
        if expert < window_count:
            half = partial_up[expert * 2 * rows : (expert + 1) * 2 * rows]
            items.append((half, "tp", "lanes"))
        received = send(items, 6 + expert)
        gate_up += [sum_of(item, got) for item, got in zip(waiting, received)]
        if expert < window_count:
            half = sum_of(items[-1], received[-1]).astype(bf16)
            half = half.reshape(2, rep_count, own, hidden_dev)
            waiting = [(half[0], "rep", "lead"), (half[1], "rep", "lead")]
    gate_up = jnp.stack(gate_up).reshape(
        window_count, 2, own // CAPACITY, CAPACITY, hidden_dev
    ).transpose(1, 2, 0, 3, 4)
    gate_up = gate_up.reshape(2, window_count * own, hidden_dev)
    own_slots = window_count * own
    gate_own = lax.dynamic_slice_in_dim(slot_gate.reshape(-1), rep_index * own_slots, own_slots, 0)
    hidden = (
        gate_own.astype(f32)[:, None]
        * jax.nn.silu(gate_up[0])
        * gate_up[1]
    )
    expert_hidden = hidden.astype(bf16)
    return (mamba_out, conv_next, ssm_next, expert_hidden)


def solution(mesh):
    in_specs = (
        P(("rep", "tp"), None),
        P(None, "rep", "tp"),
        P("rep", None, "tp"),
        P(None, ("rep", "tp")),
        P(None, ("rep", "tp")),
        P(None, ("rep", "tp")),
        P(("rep", "tp")),
        P(None, ("rep", "tp")),
        P(("rep", "tp"), None, None),
        P("tp", "rep"),
        P(("rep", "tp"), None),
        P(None, ("rep", "tp")),
        P(("rep", "tp"), None),
        P(("rep", "tp"), None, None, None),
        P(("rep", "tp"), None),
    )
    out_specs = (P(("rep", "tp"), None), P(None, "rep", "tp"), P("rep", None, "tp"), P("rep", "tp"))
    return jax.shard_map(shards, mesh=mesh, in_specs=in_specs, out_specs=out_specs, check_vma=False)
```
